32 devices in a mesh: ep: 4 (over y, core), fsdp: 8 (over z, x).
Axes of the slice: x: 2, y: 2, z: 4, core: 2. Of those that a mesh axis runs over, the one named last changes fastest.
Arguments:
- w_down: float32 [16, 6400, 4096], P('ep', None, 'fsdp'), may hold values from -0.109375 to 0.109375
- router_weight: float32 [4096, 16], P('fsdp', 'ep'), may hold values from -0.09375 to 0.09375
- router_gain: float32 [4096], P('fsdp'), may hold values from 0.25 to 1.75
Outputs:
- serve_down: bfloat16 [16, 6400, 4096], P('ep', 'fsdp')
- scale_down: float32 [16, 6400], P('ep', 'fsdp')
- serve_router: bfloat16 [4096, 16], replicated
The draws below stay inside these ranges and needn't reach their ends.
All inputs are finite; a program needn't handle non-finite values.
Results may differ from the reference program's by a relative error of at most 0.001.
Values may be sent and summed in bfloat16 or wider, within the bound.
A program may use at most 192 MiB of HBM per device.

```python
import jax
import jax.numpy as jnp
from jax import lax

EXPERTS = 16
D_MODEL = 4096
D_EXPERT = 6400


def strengthened(entries, key, source, target, parts, factor):
    def block_of(axis_at):
        return (jnp.arange(entries.shape[axis_at]) // (entries.shape[axis_at] // parts)).reshape((-1,) + (1,) * (entries.ndim - 1 - axis_at))

    near = jax.random.permutation(key, parts)[block_of(target)]
    second = (block_of(target) + parts // 2) % parts
    return jnp.where((block_of(source) == near) | (block_of(source) == second), factor * entries, entries)


def shard_levels(stream_key, extent, cuts, low, high):
    gain = 1.0
    for position, parts in cuts:
        heights = jax.random.uniform(jax.random.fold_in(jax.random.fold_in(stream_key, 6), position), (parts,), jnp.float32, low / len(cuts), high / len(cuts))
        gain = gain * jnp.repeat(jnp.exp(heights), extent[position] // parts).reshape((-1,) + (1,) * (len(extent) - 1 - position))
    return gain


def scatter_about(rng, extent, width, limit, pieces=(), held_as=jnp.bfloat16):
    entries = width * jax.random.normal(rng, extent, jnp.float32)
    if pieces:
        entries = entries * shard_levels(rng, extent, pieces, -0.22, 0.18)
    return jnp.clip(entries, -limit, limit).astype(held_as)


def heavy_noise(own_key, dims, deviation, limit, shards, heavy, held_as=jnp.bfloat16):
    array = deviation * jax.random.normal(own_key, dims, jnp.float32)
    if shards:
        array = array * shard_levels(own_key, dims, shards, -0.22, 0.18)
    return jnp.clip(strengthened(array, jax.random.fold_in(own_key, 3), *heavy), -limit, limit).astype(held_as)


def setup_inputs(seed: int = 0) -> dict:
    arg_keys = jax.random.split(jax.random.key(seed), 4)
    return {
        "w_down": heavy_noise(arg_keys[0], (EXPERTS, D_EXPERT, D_MODEL), D_EXPERT ** -0.5, 0.109375, ((0, 4), (2, 8)), (2, 1, 8, 2.0), jnp.float32),
        "router_weight": scatter_about(arg_keys[1], (D_MODEL, EXPERTS), D_MODEL ** -0.5, 0.09375, ((0, 8), (1, 4)), jnp.float32),
        "router_gain": jnp.clip(1.0 + 0.15 * jax.random.normal(arg_keys[2], (D_MODEL,), jnp.float32), 0.25, 1.75),
    }


def reference(w_down, router_weight, router_gain):
    scale_down = jnp.sqrt(lax.optimization_barrier(jnp.sum(w_down * w_down, axis=2)))
    serve_down = (w_down / jnp.expand_dims(scale_down, 2)).astype(jnp.bfloat16)
    serve_router = (router_weight * router_gain[:, None]).astype(jnp.bfloat16)
    return (serve_down, scale_down, serve_router)
```

```python
import functools

import jax
import jax.numpy as jnp
from jax import lax
from jax.experimental import pallas as pl
from jax.experimental.pallas import tpu as pltpu
from jax.sharding import PartitionSpec as P

LANES = 128
MESH = pl.DeviceIdType.MESH


def each(count, f):
    def step(i, c):
        f(i)
        return c
    lax.fori_loop(0, count, step, 0)


def ceil_to(a, b):
    return -(-a // b) * b


def kernel(n, m, w, rw, gain, o, sc, router,
           xbuf, sbuf, own, early, early_inv, part, recvp, mine, scales,
           rw_v, gain_v, rbuf, rwide, router_v, sc_v, sc_rows,
           load_a, load_b, arg_sem, esend, erecv, psend, precv, ssend, srecv,
           asend, arecv, bsend, brecv, own_sem, rsend, rrecv, gsend, grecv, out_sem):
    experts, rows, cols = w.shape
    block = rows // n
    tiles = -(-block // LANES)
    padded = part.shape[2]
    head = min(LANES, block)
    rest = block - head
    half = n // 2
    me = lax.axis_index("fsdp")
    group = lax.axis_index("ep")
    side = me // half
    mycols = pl.ds(pl.multiple_of(me * cols, LANES), cols)

    def peer(j):
        c = j // half
        return ((1 - side) * (1 - c) + side * c) * half + (me + j + c) % half

    def mate(j):
        return (group + j + 1) % m

    def send(src, dst, s, r, **to):
        return pltpu.make_async_remote_copy(
            src_ref=src, dst_ref=dst, send_sem=s, recv_sem=r,
            device_id=to, device_id_type=MESH)

    def load_head(d):
        return pltpu.make_async_copy(
            w.at[0, pl.ds(pl.multiple_of(d * block, 8), head), :],
            xbuf.at[d, pl.ds(0, head), :], load_a.at[d])

    def load_rest(d):
        return pltpu.make_async_copy(
            w.at[0, pl.ds(pl.multiple_of(d * block + head, 8), rest), :],
            xbuf.at[d, pl.ds(head, rest), :], load_b.at[d])

    def load(e, d):
        return pltpu.make_async_copy(
            w.at[e, pl.ds(pl.multiple_of(d * block, 8), block), :], xbuf.at[d], load_b.at[d])

    def early_copy(to, source):
        return send(early.at[me], early.at[source], esend.at[to], erecv.at[source], fsdp=to)

    def sums(e, to, source):
        return send(part.at[e, to], recvp.at[e, source],
                    psend.at[e, to], precv.at[e, source], fsdp=to)

    def scale_copy(e, to, source):
        return send(mine.at[e], scales.at[e, source],
                    ssend.at[e, to], srecv.at[e, source], fsdp=to)

    def bulk_head(j, to, source):
        return send(sbuf.at[0, j, pl.ds(0, head), :],
                    o.at[0, pl.ds(0, head), pl.ds(pl.multiple_of(source * cols, LANES), cols)],
                    asend.at[j], arecv.at[source], fsdp=to)

    def bulk_rest(j, to, source):
        return send(sbuf.at[0, j, pl.ds(head, rest), :],
                    o.at[0, pl.ds(head, rest), pl.ds(pl.multiple_of(source * cols, LANES), cols)],
                    bsend.at[0, j], brecv.at[0, source], fsdp=to)

    def bulk(e, j, to, source):
        return send(sbuf.at[e, j],
                    o.at[e, :, pl.ds(pl.multiple_of(source * cols, LANES), cols)],
                    bsend.at[e, j], brecv.at[e, source], fsdp=to)

    def local(e):
        return pltpu.make_async_copy(own.at[e % 2], o.at[e, :, mycols], own_sem.at[e % 2])

    width = rw.shape[1]
    rcols = width

    def router_copy(to, source):
        where = pl.ds(pl.multiple_of(source * rcols, LANES), rcols)
        return send(rbuf.at[group, :, where], rbuf.at[group, :, where],
                    rsend.at[to], rrecv.at[source], fsdp=to)

    def group_copy(to, source):
        return send(rbuf.at[source], rbuf.at[source], gsend.at[to], grecv.at[source], ep=to)

    get_rw = pltpu.make_async_copy(rw, rw_v, arg_sem.at[0])
    get_gain = pltpu.make_async_copy(gain, gain_v, arg_sem.at[1])

    barrier = pltpu.get_barrier_semaphore()
    each(n - 1, lambda j: pl.semaphore_signal(
        barrier, inc=1, device_id={"fsdp": peer(j)}, device_id_type=MESH))
    each(m - 1, lambda j: pl.semaphore_signal(
        barrier, inc=1, device_id={"ep": mate(j)}, device_id_type=MESH))

    each(n, lambda d: load_head(d).start())
    get_rw.start()
    get_gain.start()
    if rest:
        each(n, lambda d: load_rest(d).start())

    def row_sums(d, start, count):
        x = xbuf[d, start:start + count, :]
        y = x * x
        acc = y[:, :LANES]
        for c in range(LANES, cols, LANES):
            acc = acc + y[:, c:c + LANES]
        if count < LANES:
            acc = jnp.concatenate([acc, jnp.zeros((LANES - count, LANES), jnp.float32)], axis=0)
        return jnp.sum(acc.T, axis=0, keepdims=True)

    def scaled(d, inverse, start, count, store):
        factor = jnp.broadcast_to(inverse, (LANES, LANES)).T[:count]
        for c in range(0, cols, LANES):
            x = xbuf[d, start:start + count, c:c + LANES]
            store(start, count, c, (x * factor).astype(jnp.bfloat16))

    spans = [(t, t * LANES, min(LANES, block - t * LANES)) for t in range(tiles)]
    late = [span for span in spans if span[1] >= head]

    def begin(d):
        load_head(d).wait()
        early[me, pl.ds(d, 1), :] = row_sums(d, 0, head)

    each(n, begin)

    pl.semaphore_wait(barrier, n - 1 + m - 1)
    each(n - 1, lambda j: early_copy(peer(j), me).start())

    get_rw.wait()
    get_gain.wait()
    rbuf[group, :, pl.ds(pl.multiple_of(me * rcols, LANES), rcols)] = (
        rw_v[...] * gain_v[...]).astype(jnp.bfloat16)

    each(n - 1, lambda j: early_copy(peer(j), peer(j)).wait_recv())
    early_total = early[0]
    for s in range(1, n):
        early_total = early_total + early[s]
    early_inv[0] = 1.0 / jnp.sqrt(early_total)
    early_inv[1] = early_total

    def send_head(j):
        d = peer(j)

        def store(start, count, c, value):
            sbuf[0, j, start:start + count, c:c + LANES] = value

        scaled(d, early_inv[0, pl.ds(d, 1), :], 0, head, store)
        bulk_head(j, d, me).start()

    each(n - 1, send_head)
    each(n - 1, lambda j: router_copy(peer(j), me).start())

    def partial(e, d, which):
        found = [jnp.zeros((1, LANES), jnp.float32)] * (tiles - len(which))
        found += [row_sums(d, start, count) for _, start, count in which]
        if padded > tiles:
            found.append(jnp.zeros((padded - tiles, LANES), jnp.float32))
        part[e, d] = jnp.concatenate(found, axis=0)

    def add_up(e):
        def add(j, total):
            source = peer(j)
            sums(e, source, source).wait_recv()
            return total + recvp[e, source]

        return lax.fori_loop(0, n - 1, add, part[e, me])

    def publish(e, total):
        scale = jnp.sqrt(total)
        inverse = 1.0 / scale
        mine[e] = inverse
        scales[e, me] = inverse
        for t, start, count in spans:
            sc_rows[e, :, start:start + count] = scale[t:t + 1, :count]
        each(n - 1, lambda j: scale_copy(e, peer(j), me).start())

    def keep(e):
        def store(start, count, c, value):
            own[e % 2, start:start + count, c:c + LANES] = value

        inverse = scales[e, me]
        for t, start, count in spans:
            scaled(me, inverse[t:t + 1, :], start, count, store)
        local(e).start()

    def spread(e, j, which):
        d = peer(j)
        scale_copy(e, d, d).wait_recv()

        def store(start, count, c, value):
            sbuf[e, j, start:start + count, c:c + LANES] = value

        inverse = scales[e, d]
        for t, start, count in which:
            scaled(d, inverse[t:t + 1, :], start, count, store)

    def first_sums(j):
        d = peer(j)
        if rest:
            load_rest(d).wait()
        partial(0, d, late)
        sums(0, d, me).start()

    each(n - 1, first_sums)
    if rest:
        load_rest(me).wait()
    partial(0, me, late)
    total = add_up(0)
    first_row = lax.broadcasted_iota(jnp.int32, total.shape, 0) == 0
    publish(0, jnp.where(first_row, early_inv[1, pl.ds(me, 1), :], total))

    def first_spread(j):
        spread(0, j, late)
        if experts > 1:
            load(1, peer(j)).start()
        if rest:
            bulk_rest(j, peer(j), me).start()

    each(n - 1, first_spread)
    keep(0)
    if experts > 1:
        load(1, me).start()

    each(n - 1, lambda j: router_copy(peer(j), peer(j)).wait_recv())
    each(m - 1, lambda j: group_copy(mate(j), group).start())

    def expert(k):
        e = k + 1

        def some_sums(j):
            d = peer(j)
            load(e, d).wait()
            partial(e, d, spans)
            sums(e, d, me).start()

        each(n - 1, some_sums)
        load(e, me).wait()
        partial(e, me, spans)
        publish(e, add_up(e))

        @pl.when(e >= 2)
        def _():
            local(e - 2).wait()

        def some_spread(j):
            spread(e, j, spans)

            @pl.when(e + 1 < experts)
            def _():
                load(e + 1, peer(j)).start()

            bulk(e, j, peer(j), me).start()

        each(n - 1, some_spread)
        keep(e)

        @pl.when(e + 1 < experts)
        def _():
            load(e + 1, me).start()

    if experts > 1:
        each(experts - 1, expert)

    each(m - 1, lambda j: group_copy(mate(j), mate(j)).wait_recv())
    lines = rbuf.shape[1]
    for g in range(m):
        rwide[g * lines:(g + 1) * lines, :] = rbuf[g].astype(jnp.float32)
    router_v[...] = rwide[...].astype(jnp.bfloat16)
    for e in range(experts):
        sc_v[e:e + 1, :] = sc_rows[e]
    put_router = pltpu.make_async_copy(router_v, router, out_sem.at[0])
    put_scale = pltpu.make_async_copy(sc_v, sc, out_sem.at[1])
    put_router.start()
    put_scale.start()

    for e in range(max(0, experts - 2), experts):
        local(e).wait()

    def finish(j):
        d = peer(j)
        early_copy(d, me).wait_send()
        router_copy(d, me).wait_send()
        bulk_head(j, d, me).wait_send()
        bulk_head(j, d, d).wait_recv()
        if rest:
            bulk_rest(j, d, me).wait_send()
            bulk_rest(j, d, d).wait_recv()
        sums(0, d, me).wait_send()
        scale_copy(0, d, me).wait_send()

        def more(k):
            e = k + 1
            sums(e, d, me).wait_send()
            scale_copy(e, d, me).wait_send()
            bulk(e, j, d, me).wait_send()
            bulk(e, j, d, d).wait_recv()

        if experts > 1:
            each(experts - 1, more)

    each(n - 1, finish)
    each(m - 1, lambda j: group_copy(mate(j), group).wait_send())
    put_router.wait()
    put_scale.wait()


def exchange(n, m, w, rw, gain):
    experts, rows, cols = w.shape
    lines, width = rw.shape
    block = rows // n
    tiles = -(-block // LANES)
    padded = ceil_to(tiles, 8)
    depth = ceil_to(n, 8)
    dma = pltpu.SemaphoreType.DMA
    f32, bf16 = jnp.float32, jnp.bfloat16
    buffers = [
        ((n, block, cols), f32),
        ((experts, n - 1, block, cols), bf16),
        ((2, block, cols), bf16),
        ((n, depth, LANES), f32),
        ((2, depth, LANES), f32),
        ((experts, n, padded, LANES), f32),
        ((experts, n, padded, LANES), f32),
        ((experts, padded, LANES), f32),
        ((experts, n, padded, LANES), f32),
        ((lines, width), f32),
        ((1, width), f32),
        ((m, lines, n * width), bf16),
        ((m * lines, n * width), f32),
        ((m * lines, n * width), bf16),
        ((experts, block), f32),
        ((experts, 1, block), f32),
    ]
    size = sum(functools.reduce(lambda a, b: a * b, s) * jnp.dtype(t).itemsize for s, t in buffers)
    return pl.pallas_call(
        functools.partial(kernel, n, m),
        out_shape=(
            jax.ShapeDtypeStruct((experts, block, n * cols), bf16),
            jax.ShapeDtypeStruct((experts, block), f32),
            jax.ShapeDtypeStruct((m * lines, n * width), bf16),
        ),
        in_specs=[pl.BlockSpec(memory_space=pltpu.HBM)] * 3,
        out_specs=(pl.BlockSpec(memory_space=pl.ANY),) * 3,
        scratch_shapes=[pltpu.VMEM(s, t) for s, t in buffers] + [
            dma((n,)), dma((n,)), dma((2,)), dma((n,)), dma((n,)),
            dma((experts, n)), dma((experts, n)), dma((experts, n)), dma((experts, n)),
            dma((n,)), dma((n,)), dma((experts, n)), dma((experts, n)), dma((2,)),
            dma((n,)), dma((n,)), dma((m,)), dma((m,)), dma((2,)),
        ],
        compiler_params=pltpu.CompilerParams(
            collective_id=0, has_side_effects=True,
            vmem_limit_bytes=ceil_to(size + 6 * 512 * 1024, 512 * 1024)),
    )(w, rw, gain)


def body(n, m, w_down, router_weight, router_gain):
    serve_down, scale_down, router = exchange(n, m, w_down, router_weight.T, router_gain[None, :])
    return (serve_down, scale_down, router.T)


def solution(mesh):
    in_specs = (P("ep", None, "fsdp"), P("fsdp", "ep"), P("fsdp"))
    out_specs = (P("ep", "fsdp", None), P("ep", "fsdp"), P())
    return jax.shard_map(
        functools.partial(body, mesh.shape["fsdp"], mesh.shape["ep"]), mesh=mesh,
        in_specs=in_specs, out_specs=out_specs, check_vma=False)
```

```python
import functools

import jax
import jax.numpy as jnp
from jax import lax
from jax.experimental import pallas as pl
from jax.experimental.pallas import tpu as pltpu
from jax.sharding import PartitionSpec as P

LANES = 128
TAIL_START = 32
VMEM_BYTES = 67043328
MESH = pl.DeviceIdType.MESH


def each(count, f):
    def step(i, c):
        f(i)
        return c
    lax.fori_loop(0, count, step, 0)


def cuts(rows):
    first, second = ceil_to(rows * 48 // 128, 16), ceil_to(rows * 32 // 128, 16)
    return [(0, first), (first, second), (first + second, rows - first - second)]


def ceil_to(a, b):
    return -(-a // b) * b


def kernel(n, m, w, rw, gain, o, sc, router, tail,
           xbuf, sbuf, own, early, totals, part, recvp, mine, scales,
           rw_v, gain_v, rbuf, rwide, router_v, sc_v, sc_rows,
           head_sem, load_sem, arg_sem, esend, erecv, psend, precv, ssend, srecv,
           hsend, hrecv, bsend, brecv, own_sem, rsend, rrecv, gsend, grecv, out_sem):
    experts, rows, cols = w.shape
    block = rows // n
    tiles = -(-block // LANES)
    padded = part.shape[2]
    spans = [(t, t * LANES, min(LANES, block - t * LANES)) for t in range(tiles)]
    leads = early.shape[0]
    begin = min(leads * LANES, block)
    rest = block - begin
    late = spans[leads:]
    width = rw.shape[1]
    last = experts - 2 if experts > 2 else 1
    far = n // 2 - 1
    keep_back = tail.shape[0]
    short = block - keep_back
    me = lax.axis_index("fsdp")
    group = lax.axis_index("ep")

    pieces = cuts(min(LANES, block))

    def peer(j):
        return (me + 1 + j) % n

    def mate(j):
        return (group + 1 + j) % m

    def block_of(source):
        return pl.ds(pl.multiple_of(source * cols, LANES), cols)

    def send(src, dst, s, r, **to):
        return pltpu.make_async_remote_copy(
            src_ref=src, dst_ref=dst, send_sem=s, recv_sem=r,
            device_id=to, device_id_type=MESH)

    def load_part(d, start, count, sem):
        return pltpu.make_async_copy(
            w.at[0, pl.ds(pl.multiple_of(d * block + start, 8), count), :],
            xbuf.at[0, d, pl.ds(start, count), :], sem)

    def load_lead(t, d):
        return load_part(d, spans[t][1], spans[t][2], head_sem.at[t, d])

    def load_rest(d):
        return load_part(d, begin, rest, load_sem.at[0, d])

    def load(e, g, d):
        return pltpu.make_async_copy(
            w.at[e, pl.ds(pl.multiple_of(d * block, 8), block), :],
            xbuf.at[g, d], load_sem.at[g, d])

    def early_copy(t, to, source):
        return send(early.at[t, me], early.at[t, source],
                    esend.at[t, to], erecv.at[t, source], fsdp=to)

    def sums(e, to, source):
        return send(part.at[e, to], recvp.at[e, source],
                    psend.at[e, to], precv.at[e, source], fsdp=to)

    def scale_copy(e, to, source):
        return send(mine.at[e], scales.at[e, source],
                    ssend.at[e, to], srecv.at[e, source], fsdp=to)

    def piece_copy(p, j, to, source):
        start, count = pieces[p]
        return send(sbuf.at[0, j, pl.ds(start, count), :],
                    o.at[0, pl.ds(start, count), block_of(source)],
                    hsend.at[p, j], hrecv.at[p, source], fsdp=to)

    def bulk_rest(j, to, source):
        return send(sbuf.at[0, j, pl.ds(begin, rest), :],
                    o.at[0, pl.ds(begin, rest), block_of(source)],
                    bsend.at[0, j], brecv.at[0, source], fsdp=to)

    def bulk(e, j, to, source):
        return send(sbuf.at[e, j], o.at[e, :, block_of(source)],
                    bsend.at[e, j], brecv.at[e, source], fsdp=to)

    def bulk_short(to, source):
        return send(sbuf.at[last, far, pl.ds(0, short), :],
                    o.at[last, pl.ds(0, short), block_of(source)],
                    bsend.at[last, far], brecv.at[last, source], fsdp=to)

    def to_tail():
        return pltpu.make_async_copy(
            sbuf.at[last, far, pl.ds(short, keep_back), :], tail, out_sem.at[2])

    def local(e, s):
        return pltpu.make_async_copy(own.at[s], o.at[e, :, block_of(me)], own_sem.at[s])

    def router_copy(to, source):
        where = pl.ds(pl.multiple_of(source * width, LANES), width)
        return send(rbuf.at[group, :, where], rbuf.at[group, :, where],
                    rsend.at[to], rrecv.at[source], fsdp=to)

    def group_copy(to, source):
        return send(rbuf.at[source], rbuf.at[source], gsend.at[to], grecv.at[source], ep=to)

    def row_sums(g, d, start, count):
        x = xbuf[g, d, start:start + count, :]
        y = x * x
        acc = y[:, :LANES]
        for c in range(LANES, cols, LANES):
            acc = acc + y[:, c:c + LANES]
        if count < LANES:
            acc = jnp.concatenate([acc, jnp.zeros((LANES - count, LANES), jnp.float32)], axis=0)
        return jnp.sum(acc.T, axis=0, keepdims=True)

    def scaled(g, d, inverse, t, start, count, store):
        first = start - t * LANES
        factor = jnp.broadcast_to(inverse, (LANES, LANES)).T[first:first + count]
        for c in range(0, cols, LANES):
            x = xbuf[g, d, start:start + count, c:c + LANES]
            store(start, count, c, (x * factor).astype(jnp.bfloat16))

    def into(e, j):
        def store(start, count, c, value):
            sbuf[e, j, start:start + count, c:c + LANES] = value
        return store

    get_rw = pltpu.make_async_copy(rw, rw_v, arg_sem.at[0])
    get_gain = pltpu.make_async_copy(gain, gain_v, arg_sem.at[1])

    barrier = pltpu.get_barrier_semaphore()
    each(n - 1, lambda j: pl.semaphore_signal(
        barrier, inc=1, device_id={"fsdp": peer(j)}, device_id_type=MESH))
    each(m - 1, lambda j: pl.semaphore_signal(
        barrier, inc=1, device_id={"ep": mate(j)}, device_id_type=MESH))
    for t in range(leads):
        each(n, lambda d: load_lead(t, d).start())
    get_rw.start()
    get_gain.start()
    if rest:
        each(n, lambda d: load_rest(d).start())
    if experts > 1:
        each(n, lambda d: load(1, 1, d).start())

    for t in range(leads):
        def lead_sums(d):
            load_lead(t, d).wait()
            early[t, me, pl.ds(d, 1), :] = row_sums(0, d, *spans[t][1:])

        each(n, lead_sums)
        if t == 0:
            pl.semaphore_wait(barrier, n - 1 + m - 1)
        each(n - 1, lambda j: early_copy(t, peer(j), me).start())

    get_rw.wait()
    get_gain.wait()
    rbuf[group, :, pl.ds(pl.multiple_of(me * width, LANES), width)] = (
        rw_v[...] * gain_v[...]).astype(jnp.bfloat16)

    def lead_totals(t):
        each(n - 1, lambda j: early_copy(t, peer(j), peer(j)).wait_recv())
        total = early[t, 0]
        for s in range(1, n):
            total = total + early[t, s]
        totals[t, 0] = total
        totals[t, 1] = 1.0 / jnp.sqrt(total)

    def send_piece(p):
        start, count = pieces[p]
        t = start // LANES

        def one(j):
            d = peer(j)
            scaled(0, d, totals[t, 1, pl.ds(d, 1), :], t, start, count, into(0, j))
            piece_copy(p, j, d, me).start()

        each(n - 1, one)

    lead_totals(0)
    send_piece(0)
    each(n - 1, lambda j: router_copy(peer(j), me).start())

    def partial(e, g, d, which):
        found = [jnp.zeros((1, LANES), jnp.float32)] * (tiles - len(which))
        found += [row_sums(g, d, start, count) for _, start, count in which]
        if padded > tiles:
            found.append(jnp.zeros((padded - tiles, LANES), jnp.float32))
        part[e, d] = jnp.concatenate(found, axis=0)

    def first_sums(j):
        d = peer(j)
        if rest:
            load_rest(d).wait()
            partial(0, 0, d, late)
            sums(0, d, me).start()

    each(n - 1, first_sums)
    if rest:
        load_rest(me).wait()
    partial(0, 0, me, late)

    def more_sums(k):
        e = k + 1

        def one(j):
            d = peer(j)
            load(e, 1, d).wait()
            partial(e, 1, d, spans)

            @pl.when(e + 1 < experts)
            def _():
                load(e + 1, 1, d).start()

            @pl.when(j < n - 1)
            def _():
                sums(e, d, me).start()

        each(n, one)

    if experts > 1:
        each(experts - 1, more_sums)

    for t in range(1, leads):
        lead_totals(t)
    if len(pieces) > 1:
        send_piece(1)

    def publish(e, total):
        scale = jnp.sqrt(total)
        inverse = 1.0 / scale
        mine[e] = inverse
        scales[e, me] = inverse
        for t, start, count in spans:
            sc_rows[e, :, start:start + count] = scale[t:t + 1, :count]

    def add_up(e):
        def add(j, total):
            source = peer(j)
            sums(e, source, source).wait_recv()
            return total + recvp[e, source]

        return lax.fori_loop(0, n - 1, add, part[e, me])

    total = add_up(0) if rest else part[0, me]
    row = lax.broadcasted_iota(jnp.int32, total.shape, 0)
    for t in range(leads):
        total = jnp.where(row == t, totals[t, 0, pl.ds(me, 1), :], total)
    publish(0, total)
    if rest:
        each(n - 1, lambda j: scale_copy(0, peer(j), me).start())

    def more_scales(k):
        publish(k + 1, add_up(k + 1))
        each(n - 1, lambda j: scale_copy(k + 1, peer(j), me).start())

    if experts > 1:
        each(experts - 1, more_scales)

    for p in range(2, len(pieces)):
        send_piece(p)

    def keep(e, g, s):
        def store(start, count, c, value):
            own[s, start:start + count, c:c + LANES] = value

        inverse = scales[e, me]
        for t, start, count in spans:
            scaled(g, me, inverse[t:t + 1, :], t, start, count, store)
        local(e, s).start()

    def expert_at(k):
        return (k + experts - 3) % (experts - 1) + 1

    def refill(k, d):
        if experts > 3:
            @pl.when(k + 2 < experts)
            def _():
                load(expert_at(k + 2), k % 2, d).start()

    def first_rest(j):
        d = peer(j)
        if rest:
            scale_copy(0, d, d).wait_recv()
            inverse = scales[0, d]
            for t, start, count in late:
                scaled(0, d, inverse[t:t + 1, :], t, start, count, into(0, j))
            bulk_rest(j, d, me).start()
        if experts > 2:
            load(expert_at(2), 0, d).start()

    each(n - 1, first_rest)
    keep(0, 0, 0)
    if experts > 2:
        load(expert_at(2), 0, me).start()

    each(n - 1, lambda j: router_copy(peer(j), peer(j)).wait_recv())
    each(m - 1, lambda j: group_copy(mate(j), group).start())

    def more(i):
        k = i + 1
        e = expert_at(k)
        g = k % 2

        def one(j):
            d = peer(j)
            scale_copy(e, d, d).wait_recv()

            @pl.when(k >= 2)
            def _():
                load(e, g, d).wait()

            inverse = scales[e, d]
            for t, start, count in spans:
                scaled(g, d, inverse[t:t + 1, :], t, start, count, into(e, j))
            refill(k, d)
            cut = (e == last) & (j == far)

            @pl.when(cut)
            def _():
                bulk_short(d, me).start()
                to_tail().start()

            @pl.when(jnp.logical_not(cut))
            def _():
                bulk(e, j, d, me).start()

        each(n - 1, one)

        @pl.when(k >= 2)
        def _():
            load(e, g, me).wait()
            local(e, g).wait()

        keep(e, g, g)
        refill(k, me)

    if experts > 1:
        each(experts - 1, more)

    each(m - 1, lambda j: group_copy(mate(j), mate(j)).wait_recv())
    lines = rbuf.shape[1]
    for g in range(m):
        rwide[g * lines:(g + 1) * lines, :] = rbuf[g].astype(jnp.float32)
    router_v[...] = rwide[...].astype(jnp.bfloat16)
    for e in range(experts):
        sc_v[e:e + 1, :] = sc_rows[e]
    put_router = pltpu.make_async_copy(router_v, router, out_sem.at[0])
    put_scale = pltpu.make_async_copy(sc_v, sc, out_sem.at[1])
    put_router.start()
    put_scale.start()

    for s in range(min(experts, 2)):
        local(0, s).wait()

    def finish(j):
        d = peer(j)
        for t in range(leads):
            early_copy(t, d, me).wait_send()
        router_copy(d, me).wait_send()
        for p in range(len(pieces)):
            piece_copy(p, j, d, me).wait_send()
            piece_copy(p, j, d, d).wait_recv()
        if rest:
            sums(0, d, me).wait_send()
            scale_copy(0, d, me).wait_send()
            bulk_rest(j, d, me).wait_send()
            bulk_rest(j, d, d).wait_recv()

        def other(k):
            e = k + 1
            sums(e, d, me).wait_send()
            scale_copy(e, d, me).wait_send()
            cut = (e == last) & (j == far)

            @pl.when(cut)
            def _():
                bulk_short(d, me).wait_send()
                bulk_short(d, d).wait_recv()

            @pl.when(jnp.logical_not(cut))
            def _():
                bulk(e, j, d, me).wait_send()
                bulk(e, j, d, d).wait_recv()

        if experts > 1:
            each(experts - 1, other)

    each(n - 1, finish)
    each(m - 1, lambda j: group_copy(mate(j), group).wait_send())
    put_router.wait()
    put_scale.wait()
    to_tail().wait()


def exchange(n, m, w, rw, gain):
    experts, rows, cols = w.shape
    lines, width = rw.shape
    block = rows // n
    tiles = -(-block // LANES)
    padded = ceil_to(tiles, 8)
    depth = ceil_to(n, 8)
    leads = 1
    keep_back = tail_rows(block)
    pieces = len(cuts(min(LANES, block)))
    dma = pltpu.SemaphoreType.DMA
    f32, bf16 = jnp.float32, jnp.bfloat16
    buffers = [
        ((2, n, block, cols), f32),
        ((experts, n - 1, block, cols), bf16),
        ((2, block, cols), bf16),
        ((leads, n, depth, LANES), f32),
        ((leads, 2, depth, LANES), f32),
        ((experts, n, padded, LANES), f32),
        ((experts, n, padded, LANES), f32),
        ((experts, padded, LANES), f32),
        ((experts, n, padded, LANES), f32),
        ((lines, width), f32),
        ((1, width), f32),
        ((m, lines, n * width), bf16),
        ((m * lines, n * width), f32),
        ((m * lines, n * width), bf16),
        ((experts, block), f32),
        ((experts, 1, block), f32),
    ]
    return pl.pallas_call(
        functools.partial(kernel, n, m),
        out_shape=(
            jax.ShapeDtypeStruct((experts, block, n * cols), bf16),
            jax.ShapeDtypeStruct((experts, block), f32),
            jax.ShapeDtypeStruct((m * lines, n * width), bf16),
            jax.ShapeDtypeStruct((keep_back, cols), bf16),
        ),
        in_specs=[pl.BlockSpec(memory_space=pltpu.HBM)] * 3,
        out_specs=(pl.BlockSpec(memory_space=pl.ANY),) * 4,
        scratch_shapes=[pltpu.VMEM(s, t) for s, t in buffers] + [
            dma((leads, n)), dma((2, n)), dma((2,)), dma((leads, n)), dma((leads, n)),
            dma((experts, n)), dma((experts, n)), dma((experts, n)), dma((experts, n)),
            dma((pieces, n)), dma((pieces, n)), dma((experts, n)), dma((experts, n)), dma((2,)),
            dma((n,)), dma((n,)), dma((m,)), dma((m,)), dma((3,)),
        ],
        compiler_params=pltpu.CompilerParams(
            collective_id=0, has_side_effects=True,
            vmem_limit_bytes=VMEM_BYTES),
    )(w, rw, gain)


def tail_rows(block):
    start = ceil_to(block * TAIL_START // 100, 16)
    return block - start


def settle_kernel(o, sc, router, full, sc_out, router_out, buf, sc_v, router_v, get, put):
    experts, block, _ = o.shape
    parts = get.shape[0] - 1
    rows = block * experts // (parts - 1)
    per = block // rows
    pairs = [(sc, sc_v, sc_out), (router, router_v, router_out)]

    def where(i):
        return i // per, pl.ds(pl.multiple_of(i % per * rows, 8), rows)

    def load(i):
        e, r = where(i)
        return pltpu.make_async_copy(o.at[e, r, :], buf.at[e, r, :], get.at[i])

    def save(i):
        e, r = where(i)
        return pltpu.make_async_copy(buf.at[e, r, :], full.at[e, r, :], put.at[i])

    def load_small(i):
        return pltpu.make_async_copy(pairs[i][0], pairs[i][1], get.at[parts - 1 + i])

    def save_small(i):
        return pltpu.make_async_copy(pairs[i][1], pairs[i][2], put.at[parts - 1 + i])

    each(parts - 1, lambda i: load(i).start())
    for i in range(2):
        load_small(i).start()

    def move(i):
        load(i).wait()
        save(i).start()

    each(parts - 1, move)
    for i in range(2):
        load_small(i).wait()
        save_small(i).start()
    each(parts - 1, lambda i: save(i).wait())
    for i in range(2):
        save_small(i).wait()


def settle(o, sc, router):
    experts, block, _ = o.shape
    per = max(p for p in (1, 2, 4, 5) if p == 1 or block % (16 * p) == 0)
    count = experts * per + 2
    dma = pltpu.SemaphoreType.DMA
    return pl.pallas_call(
        settle_kernel,
        out_shape=tuple(jax.ShapeDtypeStruct(a.shape, a.dtype) for a in (o, sc, router)),
        in_specs=[pl.BlockSpec(memory_space=pltpu.HBM)] * 3,
        out_specs=(pl.BlockSpec(memory_space=pltpu.HBM),) * 3,
        scratch_shapes=[pltpu.VMEM(a.shape, a.dtype) for a in (o, sc, router)] + [
            dma((count,)), dma((count,))],
        cost_estimate=pl.CostEstimate(flops=0, bytes_accessed=4 * o.size, transcendentals=0),
        compiler_params=pltpu.CompilerParams(vmem_limit_bytes=48 * 1024 * 1024),
    )(o, sc, router)


def place_kernel(n, expert, full, got, out, sem):
    del full
    rows, cols = got.shape
    source = (lax.axis_index("fsdp") + n // 2) % n
    copy = pltpu.make_async_copy(
        got, out.at[expert, pl.ds(out.shape[1] - rows, rows),
                    pl.ds(pl.multiple_of(source * cols, LANES), cols)], sem)
    copy.start()
    copy.wait()


def place(n, expert, full, got):
    return pl.pallas_call(
        functools.partial(place_kernel, n, expert),
        out_shape=jax.ShapeDtypeStruct(full.shape, full.dtype),
        in_specs=[pl.BlockSpec(memory_space=pltpu.HBM), pl.BlockSpec(memory_space=pltpu.VMEM)],
        out_specs=pl.BlockSpec(memory_space=pltpu.HBM),
        scratch_shapes=[pltpu.SemaphoreType.DMA],
        input_output_aliases={0: 0},
        compiler_params=pltpu.CompilerParams(vmem_limit_bytes=8 * 1024 * 1024),
    )(full, got)


def body(n, m, w_down, router_weight, router_gain):
    experts = w_down.shape[0]
    o, scale, router, tail = exchange(n, m, w_down, router_weight.T, router_gain[None, :])
    got = lax.ppermute(tail, "fsdp", [(i, (i + n // 2) % n) for i in range(n)])
    full, scale, router = settle(o, scale, router)
    serve_down = place(n, experts - 2 if experts > 2 else 1, full, got)
    return (serve_down, scale, router.T)


def solution(mesh):
    in_specs = (P("ep", None, "fsdp"), P("fsdp", "ep"), P("fsdp"))
    out_specs = (P("ep", "fsdp", None), P("ep", "fsdp"), P())
    return jax.shard_map(
        functools.partial(body, mesh.shape["fsdp"], mesh.shape["ep"]), mesh=mesh,
        in_specs=in_specs, out_specs=out_specs, check_vma=False)
```

```python
import functools

import jax
import jax.numpy as jnp
from jax import lax
from jax.experimental import pallas as pl
from jax.experimental.pallas import tpu as pltpu
from jax.sharding import PartitionSpec as P

LANES = 128
TAIL_START = 32
LEADS = 2
CUTS = (64, 96, 128, 160)
VMEM_BYTES = 67043328
MESH = pl.DeviceIdType.MESH


def each(count, f):
    def step(i, c):
        f(i)
        return c
    lax.fori_loop(0, count, step, 0)


def cuts(rows):
    ends = [c for c in CUTS if c < rows] + [rows]
    starts = [0] + ends[:-1]
    return [(a, b - a) for a, b in zip(starts, ends)]


def ceil_to(a, b):
    return -(-a // b) * b


def kernel(n, m, w, rw, gain, o, sc, router, tail,
           xbuf, sbuf, own, early, totals, part, recvp, pair, scales,
           rw_v, gain_v, rbuf, rwide, router_v, sc_v, sc_rows,
           head_sem, load_sem, arg_sem, esend, erecv, psend, precv, msend, mrecv, csend, crecv,
           hsend, hrecv, bsend, brecv, own_sem, rsend, rrecv, gsend, grecv, out_sem):
    experts, rows, cols = w.shape
    block = rows // n
    tiles = -(-block // LANES)
    padded = part.shape[2]
    spans = [(t, t * LANES, min(LANES, block - t * LANES)) for t in range(tiles)]
    leads = early.shape[0]
    begin = min(leads * LANES, block)
    rest = block - begin
    late = spans[leads:]
    width = rw.shape[1]
    last = experts - 2 if experts > 2 else 1
    far = n // 2 - 1
    keep_back = tail.shape[0]
    short = block - keep_back
    me = lax.axis_index("fsdp")
    group = lax.axis_index("ep")
    half = n // 2
    side, rank = me // half, me % half

    pieces = cuts(begin)

    def peer(j):
        return (me + 1 + j) % n

    def order(q):
        return (me + (1 + q)) % n

    def place_in(d):
        return (me * (n - 1) + d + n - 1) % n

    def mate(j):
        return (group + 1 + j) % m

    def block_of(source):
        return pl.ds(pl.multiple_of(source * cols, LANES), cols)

    def send(src, dst, s, r, **to):
        return pltpu.make_async_remote_copy(
            src_ref=src, dst_ref=dst, send_sem=s, recv_sem=r,
            device_id=to, device_id_type=MESH)

    def load_part(d, start, count, sem):
        return pltpu.make_async_copy(
            w.at[0, pl.ds(pl.multiple_of(d * block + start, 8), count), :],
            xbuf.at[0, d, pl.ds(start, count), :], sem)

    def load_lead(t, d):
        return load_part(d, spans[t][1], spans[t][2], head_sem.at[t, d])

    def load_rest(d):
        return load_part(d, begin, rest, load_sem.at[0, d])

    def load(e, g, d):
        return pltpu.make_async_copy(
            w.at[e, pl.ds(pl.multiple_of(d * block, 8), block), :],
            xbuf.at[g, d], load_sem.at[g, d])

    def early_copy(t, to, source):
        return send(early.at[t, me], early.at[t, source],
                    esend.at[t, to], erecv.at[t, source], fsdp=to)

    def neighbour(g):
        return side * half + g

    def sums(e, d, source):
        return send(part.at[e, d], recvp.at[e, source, d // half],
                    psend.at[e, d], precv.at[e, source * 2 + d // half],
                    fsdp=neighbour(d % half))

    def across(source):
        return send(pair.at[source], pair.at[source], msend, mrecv, fsdp=(me + half) % n)

    def scale_copy(to, source):
        return send(scales.at[source], scales.at[source],
                    csend.at[to], crecv.at[source], fsdp=neighbour(to))

    def other(j):
        return (rank + 1 + j) % half

    def piece_copy(p, j, to, source):
        start, count = pieces[p]
        return send(sbuf.at[0, j, pl.ds(start, count), :],
                    o.at[0, pl.ds(start, count), block_of(source)],
                    hsend.at[p, j], hrecv.at[p, source], fsdp=to)

    def bulk_rest(j, to, source):
        return send(sbuf.at[0, j, pl.ds(begin, rest), :],
                    o.at[0, pl.ds(begin, rest), block_of(source)],
                    bsend.at[0, j], brecv.at[0, source], fsdp=to)

    def bulk(e, j, to, source):
        return send(sbuf.at[e, j], o.at[e, :, block_of(source)],
                    bsend.at[e, j], brecv.at[e, source], fsdp=to)

    def bulk_short(to, source):
        return send(sbuf.at[last, far, pl.ds(0, short), :],
                    o.at[last, pl.ds(0, short), block_of(source)],
                    bsend.at[last, far], brecv.at[last, source], fsdp=to)

    def to_tail():
        return pltpu.make_async_copy(
            sbuf.at[last, far, pl.ds(short, keep_back), :], tail, out_sem.at[2])

    def local(e, s):
        return pltpu.make_async_copy(own.at[s], o.at[e, :, block_of(me)], own_sem.at[s])

    def router_copy(to, source):
        where = pl.ds(pl.multiple_of(source * width, LANES), width)
        return send(rbuf.at[group, :, where], rbuf.at[group, :, where],
                    rsend.at[to], rrecv.at[source], fsdp=to)

    def group_copy(to, source):
        return send(rbuf.at[source], rbuf.at[source], gsend.at[to], grecv.at[source], ep=to)

    def row_sums(g, d, start, count):
        x = xbuf[g, d, start:start + count, :]
        y = x * x
        acc = y[:, :LANES]
        for c in range(LANES, cols, LANES):
            acc = acc + y[:, c:c + LANES]
        if count < LANES:
            acc = jnp.concatenate([acc, jnp.zeros((LANES - count, LANES), jnp.float32)], axis=0)
        return jnp.sum(acc.T, axis=0, keepdims=True)

    def scaled(g, d, inverse, t, start, count, store):
        first = start - t * LANES
        factor = jnp.broadcast_to(inverse, (LANES, LANES)).T[first:first + count]
        for c in range(0, cols, LANES):
            x = xbuf[g, d, start:start + count, c:c + LANES]
            store(start, count, c, (x * factor).astype(jnp.bfloat16))

    def into(e, j):
        def store(start, count, c, value):
            sbuf[e, j, start:start + count, c:c + LANES] = value
        return store

    get_rw = pltpu.make_async_copy(rw, rw_v, arg_sem.at[0])
    get_gain = pltpu.make_async_copy(gain, gain_v, arg_sem.at[1])

    barrier = pltpu.get_barrier_semaphore()
    each(n - 1, lambda j: pl.semaphore_signal(
        barrier, inc=1, device_id={"fsdp": peer(j)}, device_id_type=MESH))
    each(m - 1, lambda j: pl.semaphore_signal(
        barrier, inc=1, device_id={"ep": mate(j)}, device_id_type=MESH))
    for t in range(leads):
        each(n, lambda d: load_lead(t, d).start())
    get_rw.start()
    get_gain.start()
    if rest:
        each(n, lambda d: load_rest(d).start())
    if experts > 1:
        each(n, lambda d: load(1, 1, d).start())

    for t in range(leads):
        def lead_sums(d):
            load_lead(t, d).wait()
            early[t, me, pl.ds(d, 1), :] = row_sums(0, d, *spans[t][1:])

        each(n, lead_sums)
        if t == 0:
            pl.semaphore_wait(barrier, n - 1 + m - 1)
        each(n - 1, lambda j: early_copy(t, peer(j), me).start())

    get_rw.wait()
    get_gain.wait()
    rbuf[group, :, pl.ds(pl.multiple_of(me * width, LANES), width)] = (
        rw_v[...] * gain_v[...]).astype(jnp.bfloat16)
    each(n - 1, lambda j: router_copy(peer(j), me).start())

    def lead_totals(t):
        each(n - 1, lambda j: early_copy(t, peer(j), peer(j)).wait_recv())
        total = early[t, 0]
        for s in range(1, n):
            total = total + early[t, s]
        totals[t, 0] = total
        totals[t, 1] = 1.0 / jnp.sqrt(total)

    def send_piece(p):
        start, count = pieces[p]
        t = start // LANES

        def one(q):
            d = order(q)
            j = place_in(d)
            scaled(0, d, totals[t, 1, pl.ds(d, 1), :], t, start, count, into(0, j))
            piece_copy(p, j, d, me).start()

        each(n - 1, one)

    lead_totals(0)
    send_piece(0)

    def partial(e, g, d, which):
        found = [jnp.zeros((1, LANES), jnp.float32)] * (tiles - len(which))
        found += [row_sums(g, d, start, count) for _, start, count in which]
        if padded > tiles:
            found.append(jnp.zeros((padded - tiles, LANES), jnp.float32))
        part[e, d] = jnp.concatenate(found, axis=0)

    def first_sums(j):
        d = peer(j)
        load_rest(d).wait()
        partial(0, 0, d, late)

        @pl.when(d % half != rank)
        def _():
            sums(0, d, rank).start()

    if rest:
        each(n, first_sums)

    def more_sums(k):
        e = k + 1

        def one(j):
            d = peer(j)
            load(e, 1, d).wait()
            partial(e, 1, d, spans)

            @pl.when(e + 1 < experts)
            def _():
                load(e + 1, 1, d).start()

            @pl.when(d % half != rank)
            def _():
                sums(e, d, rank).start()

        each(n, one)

    if experts > 1:
        each(experts - 1, more_sums)

    for t in range(1, leads):
        lead_totals(t)
    if len(pieces) > 1:
        send_piece(1)

    first_sum = 0 if rest else 1

    def add_up(i):
        e, b = first_sum + i // 2, i % 2

        def add(j, total):
            source = other(j)
            sums(e, b * half + rank, source).wait_recv()
            return total + recvp[e, source, b]

        pair[side, e, b] = lax.fori_loop(0, half - 1, add, part[e, b * half + rank])

    each(2 * (experts - first_sum), add_up)
    across(side).start()

    if len(pieces) > 2:
        send_piece(2)

    across(1 - side).wait_recv()

    def scale_of(i):
        e, b = i // 2, i % 2
        total = pair[0, e, b] + pair[1, e, b]
        row = lax.broadcasted_iota(jnp.int32, total.shape, 0)
        for t in range(leads):
            lead = totals[t, 0, pl.ds(b * half + rank, 1), :]
            total = jnp.where((row == t) & (e == 0), lead, total)
        scale = jnp.sqrt(total)
        scales[rank, e, b] = 1.0 / scale

        @pl.when(b == side)
        def _():
            for t, start, count in spans:
                sc_rows[e, :, start:start + count] = scale[t:t + 1, :count]

    each(2 * experts, scale_of)
    each(half - 1, lambda j: scale_copy(other(j), rank).start())

    for p in range(3, len(pieces)):
        send_piece(p)

    def keep(e, g, s):
        def store(start, count, c, value):
            own[s, start:start + count, c:c + LANES] = value

        inverse = scales[rank, e, side]
        for t, start, count in spans:
            scaled(g, me, inverse[t:t + 1, :], t, start, count, store)
        local(e, s).start()

    def expert_at(k):
        return (k + experts - 3) % (experts - 1) + 1

    def refill(k, d):
        if experts > 3:
            @pl.when(k + 2 < experts)
            def _():
                load(expert_at(k + 2), k % 2, d).start()

    def first_rest(q):
        d = order(q)
        j = place_in(d)
        if rest:
            inverse = scales[d % half, 0, d // half]
            for t, start, count in late:
                scaled(0, d, inverse[t:t + 1, :], t, start, count, into(0, j))
            bulk_rest(j, d, me).start()
        if experts > 2:
            load(expert_at(2), 0, d).start()

    each(half - 1, lambda j: scale_copy(other(j), other(j)).wait_recv())
    each(n - 1, first_rest)
    keep(0, 0, 0)
    if experts > 2:
        load(expert_at(2), 0, me).start()

    each(n - 1, lambda j: router_copy(peer(j), peer(j)).wait_recv())
    each(m - 1, lambda j: group_copy(mate(j), group).start())

    def more(i):
        k = i + 1
        e = expert_at(k)
        g = k % 2

        def one(q):
            d = order(q)
            j = place_in(d)

            @pl.when(k >= 2)
            def _():
                load(e, g, d).wait()

            inverse = scales[d % half, e, d // half]
            for t, start, count in spans:
                scaled(g, d, inverse[t:t + 1, :], t, start, count, into(e, j))
            refill(k, d)
            cut = (e == last) & (j == far)

            @pl.when(cut)
            def _():
                bulk_short(d, me).start()
                to_tail().start()

            @pl.when(jnp.logical_not(cut))
            def _():
                bulk(e, j, d, me).start()

        each(n - 1, one)

        @pl.when(k >= 2)
        def _():
            load(e, g, me).wait()
            local(e, g).wait()

        keep(e, g, g)
        refill(k, me)

    if experts > 1:
        each(experts - 1, more)

    each(m - 1, lambda j: group_copy(mate(j), mate(j)).wait_recv())
    lines = rbuf.shape[1]
    for g in range(m):
        rwide[g * lines:(g + 1) * lines, :] = rbuf[g].astype(jnp.float32)
    router_v[...] = rwide[...].astype(jnp.bfloat16)
    for e in range(experts):
        sc_v[e:e + 1, :] = sc_rows[e]
    put_router = pltpu.make_async_copy(router_v, router, out_sem.at[0])
    put_scale = pltpu.make_async_copy(sc_v, sc, out_sem.at[1])
    put_router.start()
    put_scale.start()

    for s in range(min(experts, 2)):
        local(0, s).wait()

    def finish(j):
        d = peer(j)
        for t in range(leads):
            early_copy(t, d, me).wait_send()
        router_copy(d, me).wait_send()
        for p in range(len(pieces)):
            piece_copy(p, j, d, me).wait_send()
            piece_copy(p, j, d, d).wait_recv()
        if rest:
            @pl.when(d % half != rank)
            def _():
                sums(0, d, rank).wait_send()

            bulk_rest(j, d, me).wait_send()
            bulk_rest(j, d, d).wait_recv()

        def others(k):
            e = k + 1

            @pl.when(d % half != rank)
            def _():
                sums(e, d, rank).wait_send()

            cut = (e == last) & (j == far)

            @pl.when(cut)
            def _():
                bulk_short(d, me).wait_send()
                bulk_short(d, d).wait_recv()

            @pl.when(jnp.logical_not(cut))
            def _():
                bulk(e, j, d, me).wait_send()
                bulk(e, j, d, d).wait_recv()

        if experts > 1:
            each(experts - 1, others)

    each(n - 1, finish)
    each(half - 1, lambda j: scale_copy(other(j), rank).wait_send())
    across(side).wait_send()
    each(m - 1, lambda j: group_copy(mate(j), group).wait_send())
    put_router.wait()
    put_scale.wait()
    to_tail().wait()


def exchange(n, m, w, rw, gain):
    experts, rows, cols = w.shape
    lines, width = rw.shape
    block = rows // n
    tiles = -(-block // LANES)
    padded = ceil_to(tiles, 8)
    depth = ceil_to(n, 8)
    leads = min(LEADS, tiles)
    keep_back = tail_rows(block)
    pieces = len(cuts(min(leads * LANES, block)))
    dma = pltpu.SemaphoreType.DMA
    f32, bf16 = jnp.float32, jnp.bfloat16
    buffers = [
        ((2, n, block, cols), f32),
        ((experts, n - 1, block, cols), bf16),
        ((2, block, cols), bf16),
        ((leads, n, depth, LANES), f32),
        ((leads, 2, depth, LANES), f32),
        ((experts, n, padded, LANES), f32),
        ((experts, n // 2, 2, padded, LANES), f32),
        ((2, experts, 2, padded, LANES), f32),
        ((n // 2, experts, 2, padded, LANES), f32),
        ((lines, width), f32),
        ((1, width), f32),
        ((m, lines, n * width), bf16),
        ((m * lines, n * width), f32),
        ((m * lines, n * width), bf16),
        ((experts, block), f32),
        ((experts, 1, block), f32),
    ]
    return pl.pallas_call(
        functools.partial(kernel, n, m),
        out_shape=(
            jax.ShapeDtypeStruct((experts, block, n * cols), bf16),
            jax.ShapeDtypeStruct((experts, block), f32),
            jax.ShapeDtypeStruct((m * lines, n * width), bf16),
            jax.ShapeDtypeStruct((keep_back, cols), bf16),
        ),
        in_specs=[pl.BlockSpec(memory_space=pltpu.HBM)] * 3,
        out_specs=(pl.BlockSpec(memory_space=pl.ANY),) * 4,
        scratch_shapes=[pltpu.VMEM(s, t) for s, t in buffers] + [
            dma((leads, n)), dma((2, n)), dma((2,)), dma((leads, n)), dma((leads, n)),
            dma((experts, n)), dma((experts, n)), dma, dma, dma((n,)), dma((n,)),
            dma((pieces, n)), dma((pieces, n)), dma((experts, n)), dma((experts, n)), dma((2,)),
            dma((n,)), dma((n,)), dma((m,)), dma((m,)), dma((3,)),
        ],
        compiler_params=pltpu.CompilerParams(
            collective_id=0, has_side_effects=True,
            vmem_limit_bytes=VMEM_BYTES),
    )(w, rw, gain)


def tail_rows(block):
    start = ceil_to(block * TAIL_START // 100, 16)
    return block - start


def settle_kernel(o, sc, router, full, sc_out, router_out, buf, sc_v, router_v, get, put):
    experts, block, _ = o.shape
    parts = get.shape[0] - 1
    rows = block * experts // (parts - 1)
    per = block // rows
    pairs = [(sc, sc_v, sc_out), (router, router_v, router_out)]

    def where(i):
        return i // per, pl.ds(pl.multiple_of(i % per * rows, 8), rows)

    def load(i):
        e, r = where(i)
        return pltpu.make_async_copy(o.at[e, r, :], buf.at[e, r, :], get.at[i])

    def save(i):
        e, r = where(i)
        return pltpu.make_async_copy(buf.at[e, r, :], full.at[e, r, :], put.at[i])

    def load_small(i):
        return pltpu.make_async_copy(pairs[i][0], pairs[i][1], get.at[parts - 1 + i])

    def save_small(i):
        return pltpu.make_async_copy(pairs[i][1], pairs[i][2], put.at[parts - 1 + i])

    each(parts - 1, lambda i: load(i).start())
    for i in range(2):
        load_small(i).start()

    def move(i):
        load(i).wait()
        save(i).start()

    each(parts - 1, move)
    for i in range(2):
        load_small(i).wait()
        save_small(i).start()
    each(parts - 1, lambda i: save(i).wait())
    for i in range(2):
        save_small(i).wait()


def settle(o, sc, router):
    experts, block, _ = o.shape
    per = max(p for p in (1, 2, 4, 5) if p == 1 or block % (16 * p) == 0)
    count = experts * per + 2
    dma = pltpu.SemaphoreType.DMA
    return pl.pallas_call(
        settle_kernel,
        out_shape=tuple(jax.ShapeDtypeStruct(a.shape, a.dtype) for a in (o, sc, router)),
        in_specs=[pl.BlockSpec(memory_space=pltpu.HBM)] * 3,
        out_specs=(pl.BlockSpec(memory_space=pltpu.HBM),) * 3,
        scratch_shapes=[pltpu.VMEM(a.shape, a.dtype) for a in (o, sc, router)] + [
            dma((count,)), dma((count,))],
        cost_estimate=pl.CostEstimate(flops=0, bytes_accessed=4 * o.size, transcendentals=0),
        compiler_params=pltpu.CompilerParams(vmem_limit_bytes=48 * 1024 * 1024),
    )(o, sc, router)


def place_kernel(n, expert, full, got, out, sem):
    del full
    rows, cols = got.shape
    source = (lax.axis_index("fsdp") + n // 2) % n
    copy = pltpu.make_async_copy(
        got, out.at[expert, pl.ds(out.shape[1] - rows, rows),
                    pl.ds(pl.multiple_of(source * cols, LANES), cols)], sem)
    copy.start()
    copy.wait()


def place(n, expert, full, got):
    return pl.pallas_call(
        functools.partial(place_kernel, n, expert),
        out_shape=jax.ShapeDtypeStruct(full.shape, full.dtype),
        in_specs=[pl.BlockSpec(memory_space=pltpu.HBM), pl.BlockSpec(memory_space=pltpu.VMEM)],
        out_specs=pl.BlockSpec(memory_space=pltpu.HBM),
        scratch_shapes=[pltpu.SemaphoreType.DMA],
        input_output_aliases={0: 0},
        compiler_params=pltpu.CompilerParams(vmem_limit_bytes=8 * 1024 * 1024),
    )(full, got)


def body(n, m, w_down, router_weight, router_gain):
    experts = w_down.shape[0]
    o, scale, router, tail = exchange(n, m, w_down, router_weight.T, router_gain[None, :])
    got = lax.ppermute(tail, "fsdp", [(i, (i + n // 2) % n) for i in range(n)])
    full, scale, router = settle(o, scale, router)
    serve_down = place(n, experts - 2 if experts > 2 else 1, full, got)
    return (serve_down, scale, router.T)


def solution(mesh):
    in_specs = (P("ep", None, "fsdp"), P("fsdp", "ep"), P("fsdp"))
    out_specs = (P("ep", "fsdp", None), P("ep", "fsdp"), P())
    return jax.shard_map(
        functools.partial(body, mesh.shape["fsdp"], mesh.shape["ep"]), mesh=mesh,
        in_specs=in_specs, out_specs=out_specs, check_vma=False)
```

```python
import functools

import jax
import jax.numpy as jnp
from jax import lax
from jax.experimental import pallas as pl
from jax.experimental.pallas import tpu as pltpu
from jax.sharding import PartitionSpec as P

LANES = 128
TAIL_START = 32
LEADS = 2
CUTS = (80, 128, 176, 224)
VMEM_BYTES = 67043328
MESH = pl.DeviceIdType.MESH


def each(count, f):
    def step(i, c):
        f(i)
        return c
    lax.fori_loop(0, count, step, 0)


def cuts(rows):
    ends = [c for c in CUTS if c < rows] + [rows]
    starts = [0] + ends[:-1]
    return [(a, b - a) for a, b in zip(starts, ends)]


def ceil_to(a, b):
    return -(-a // b) * b


def kernel(n, m, w, rw, gain, o, sc, router, tail,
           xbuf, sbuf, own, early, totals, part, recvp, pair, scales,
           rw_v, gain_v, rbuf, rwide, router_v, sc_v, sc_rows,
           head_sem, load_sem, arg_sem, esend, erecv, psend, precv, msend, mrecv, csend, crecv,
           hsend, hrecv, bsend, brecv, own_sem, rsend, rrecv, gsend, grecv, out_sem):
    experts, rows, cols = w.shape
    block = rows // n
    tiles = -(-block // LANES)
    padded = part.shape[2]
    spans = [(t, t * LANES, min(LANES, block - t * LANES)) for t in range(tiles)]
    leads = early.shape[0]
    begin = min(leads * LANES, block)
    rest = block - begin
    late = spans[leads:]
    width = rw.shape[1]
    last = experts - 2 if experts > 2 else 1
    far = n // 2 - 1
    keep_back = tail.shape[0]
    short = block - keep_back
    me = lax.axis_index("fsdp")
    group = lax.axis_index("ep")
    half = n // 2
    side, rank = me // half, me % half

    pieces = cuts(begin)

    def peer(j):
        return (me + 1 + j) % n

    def order(q):
        return (me + (1 + q)) % n

    def place_in(d):
        return (me * (n - 1) + d + n - 1) % n

    def mate(j):
        return (group + 1 + j) % m

    def block_of(source):
        return pl.ds(pl.multiple_of(source * cols, LANES), cols)

    def send(src, dst, s, r, **to):
        return pltpu.make_async_remote_copy(
            src_ref=src, dst_ref=dst, send_sem=s, recv_sem=r,
            device_id=to, device_id_type=MESH)

    def load_part(d, start, count, sem):
        return pltpu.make_async_copy(
            w.at[0, pl.ds(pl.multiple_of(d * block + start, 8), count), :],
            xbuf.at[0, d, pl.ds(start, count), :], sem)

    def load_lead(t, d):
        return load_part(d, spans[t][1], spans[t][2], head_sem.at[t, d])

    def load_rest(d):
        return load_part(d, begin, rest, load_sem.at[0, d])

    def load(e, g, d):
        return pltpu.make_async_copy(
            w.at[e, pl.ds(pl.multiple_of(d * block, 8), block), :],
            xbuf.at[g, d], load_sem.at[g, d])

    def early_copy(t, to, source):
        return send(early.at[t, me], early.at[t, source],
                    esend.at[t, to], erecv.at[t, source], fsdp=to)

    def neighbour(g):
        return side * half + g

    def sums(e, d, source):
        return send(part.at[e, d], recvp.at[e, source, d // half],
                    psend.at[e, d], precv.at[e, source * 2 + d // half],
                    fsdp=neighbour(d % half))

    def across(source):
        return send(pair.at[source], pair.at[source], msend, mrecv, fsdp=(me + half) % n)

    def scale_copy(to, source):
        return send(scales.at[source], scales.at[source],
                    csend.at[to], crecv.at[source], fsdp=neighbour(to))

    def other(j):
        return (rank + 1 + j) % half

    def piece_copy(p, j, to, source):
        start, count = pieces[p]
        return send(sbuf.at[0, j, pl.ds(start, count), :],
                    o.at[0, pl.ds(start, count), block_of(source)],
                    hsend.at[p, j], hrecv.at[p, source], fsdp=to)

    def bulk_rest(j, to, source):
        return send(sbuf.at[0, j, pl.ds(begin, rest), :],
                    o.at[0, pl.ds(begin, rest), block_of(source)],
                    bsend.at[0, j], brecv.at[0, source], fsdp=to)

    def bulk(e, j, to, source):
        return send(sbuf.at[e, j], o.at[e, :, block_of(source)],
                    bsend.at[e, j], brecv.at[e, source], fsdp=to)

    def bulk_short(to, source):
        return send(sbuf.at[last, far, pl.ds(0, short), :],
                    o.at[last, pl.ds(0, short), block_of(source)],
                    bsend.at[last, far], brecv.at[last, source], fsdp=to)

    def to_tail():
        return pltpu.make_async_copy(
            sbuf.at[last, far, pl.ds(short, keep_back), :], tail, out_sem.at[2])

    def local(e, s):
        return pltpu.make_async_copy(own.at[s], o.at[e, :, block_of(me)], own_sem.at[s])

    def router_copy(to, source):
        where = pl.ds(pl.multiple_of(source * width, LANES), width)
        return send(rbuf.at[group, :, where], rbuf.at[group, :, where],
                    rsend.at[to], rrecv.at[source], fsdp=to)

    def group_copy(to, source):
        return send(rbuf.at[source], rbuf.at[source], gsend.at[to], grecv.at[source], ep=to)

    def row_sums(g, d, start, count):
        x = xbuf[g, d, start:start + count, :]
        y = x * x
        acc = y[:, :LANES]
        for c in range(LANES, cols, LANES):
            acc = acc + y[:, c:c + LANES]
        if count < LANES:
            acc = jnp.concatenate([acc, jnp.zeros((LANES - count, LANES), jnp.float32)], axis=0)
        return jnp.sum(acc.T, axis=0, keepdims=True)

    def scaled(g, d, inverse, t, start, count, store):
        first = start - t * LANES
        factor = jnp.broadcast_to(inverse, (LANES, LANES)).T[first:first + count]
        for c in range(0, cols, LANES):
            x = xbuf[g, d, start:start + count, c:c + LANES]
            store(start, count, c, (x * factor).astype(jnp.bfloat16))

    def into(e, j):
        def store(start, count, c, value):
            sbuf[e, j, start:start + count, c:c + LANES] = value
        return store

    get_rw = pltpu.make_async_copy(rw, rw_v, arg_sem.at[0])
    get_gain = pltpu.make_async_copy(gain, gain_v, arg_sem.at[1])

    barrier = pltpu.get_barrier_semaphore()
    each(n - 1, lambda j: pl.semaphore_signal(
        barrier, inc=1, device_id={"fsdp": peer(j)}, device_id_type=MESH))
    each(m - 1, lambda j: pl.semaphore_signal(
        barrier, inc=1, device_id={"ep": mate(j)}, device_id_type=MESH))
    for t in range(leads):
        each(n, lambda d: load_lead(t, d).start())
    get_rw.start()
    get_gain.start()
    if rest:
        each(n, lambda d: load_rest(d).start())
    if experts > 1:
        each(n, lambda d: load(1, 1, d).start())

    for t in range(leads):
        def lead_sums(d):
            load_lead(t, d).wait()
            early[t, me, pl.ds(d, 1), :] = row_sums(0, d, *spans[t][1:])

        each(n, lead_sums)
        if t == 0:
            pl.semaphore_wait(barrier, n - 1 + m - 1)
        each(n - 1, lambda j: early_copy(t, peer(j), me).start())

    get_rw.wait()
    get_gain.wait()
    rbuf[group, :, pl.ds(pl.multiple_of(me * width, LANES), width)] = (
        rw_v[...] * gain_v[...]).astype(jnp.bfloat16)
    each(n - 1, lambda j: router_copy(peer(j), me).start())

    def lead_totals(t):
        each(n - 1, lambda j: early_copy(t, peer(j), peer(j)).wait_recv())
        total = early[t, 0]
        for s in range(1, n):
            total = total + early[t, s]
        totals[t, 0] = total
        totals[t, 1] = 1.0 / jnp.sqrt(total)

    def send_piece(p):
        start, count = pieces[p]
        t = start // LANES

        def one(q):
            d = order(q)
            j = place_in(d)
            scaled(0, d, totals[t, 1, pl.ds(d, 1), :], t, start, count, into(0, j))
            piece_copy(p, j, d, me).start()

        each(n - 1, one)

    lead_totals(0)
    send_piece(0)

    def partial(e, g, d, which):
        found = [jnp.zeros((1, LANES), jnp.float32)] * (tiles - len(which))
        found += [row_sums(g, d, start, count) for _, start, count in which]
        if padded > tiles:
            found.append(jnp.zeros((padded - tiles, LANES), jnp.float32))
        part[e, d] = jnp.concatenate(found, axis=0)

    def first_sums(j):
        d = peer(j)
        load_rest(d).wait()
        partial(0, 0, d, late)

        @pl.when(d % half != rank)
        def _():
            sums(0, d, rank).start()

    if rest:
        each(n, first_sums)

    def more_sums(k):
        e = k + 1

        def one(j):
            d = peer(j)
            load(e, 1, d).wait()
            partial(e, 1, d, spans)

            @pl.when(e + 1 < experts)
            def _():
                load(e + 1, 1, d).start()

            @pl.when(d % half != rank)
            def _():
                sums(e, d, rank).start()

        each(n, one)

    if experts > 1:
        each(experts - 1, more_sums)

    for t in range(1, leads):
        lead_totals(t)
    if len(pieces) > 1:
        send_piece(1)

    first_sum = 0 if rest else 1

    def add_up(i):
        e, b = first_sum + i // 2, i % 2

        def add(j, total):
            source = other(j)
            sums(e, b * half + rank, source).wait_recv()
            return total + recvp[e, source, b]

        pair[side, e, b] = lax.fori_loop(0, half - 1, add, part[e, b * half + rank])

    each(2 * (experts - first_sum), add_up)
    across(side).start()

    if len(pieces) > 2:
        send_piece(2)

    across(1 - side).wait_recv()

    def scale_of(i):
        e, b = i // 2, i % 2
        total = pair[0, e, b] + pair[1, e, b]
        row = lax.broadcasted_iota(jnp.int32, total.shape, 0)
        for t in range(leads):
            lead = totals[t, 0, pl.ds(b * half + rank, 1), :]
            total = jnp.where((row == t) & (e == 0), lead, total)
        scale = jnp.sqrt(total)
        scales[rank, e, b] = 1.0 / scale

        @pl.when(b == side)
        def _():
            for t, start, count in spans:
                sc_rows[e, :, start:start + count] = scale[t:t + 1, :count]

    each(2 * experts, scale_of)
    each(half - 1, lambda j: scale_copy(other(j), rank).start())

    for p in range(3, len(pieces)):
        send_piece(p)

    def keep(e, g, s):
        def store(start, count, c, value):
            own[s, start:start + count, c:c + LANES] = value

        inverse = scales[rank, e, side]
        for t, start, count in spans:
            scaled(g, me, inverse[t:t + 1, :], t, start, count, store)
        local(e, s).start()

    def expert_at(k):
        return (k + experts - 3) % (experts - 1) + 1

    def refill(k, d):
        if experts > 3:
            @pl.when(k + 2 < experts)
            def _():
                load(expert_at(k + 2), k % 2, d).start()

    def first_rest(q):
        d = order(q)
        j = place_in(d)
        if rest:
            inverse = scales[d % half, 0, d // half]
            for t, start, count in late:
                scaled(0, d, inverse[t:t + 1, :], t, start, count, into(0, j))
            bulk_rest(j, d, me).start()
        if experts > 2:
            load(expert_at(2), 0, d).start()

    each(half - 1, lambda j: scale_copy(other(j), other(j)).wait_recv())
    each(n - 1, first_rest)
    keep(0, 0, 0)
    if experts > 2:
        load(expert_at(2), 0, me).start()

    each(n - 1, lambda j: router_copy(peer(j), peer(j)).wait_recv())
    each(m - 1, lambda j: group_copy(mate(j), group).start())

    def more(i):
        k = i + 1
        e = expert_at(k)
        g = k % 2

        def one(q):
            d = order(q)
            j = place_in(d)

            @pl.when(k >= 2)
            def _():
                load(e, g, d).wait()

            inverse = scales[d % half, e, d // half]
            for t, start, count in spans:
                scaled(g, d, inverse[t:t + 1, :], t, start, count, into(e, j))
            refill(k, d)
            cut = (e == last) & (j == far)

            @pl.when(cut)
            def _():
                bulk_short(d, me).start()
                to_tail().start()

            @pl.when(jnp.logical_not(cut))
            def _():
                bulk(e, j, d, me).start()

        each(n - 1, one)

        @pl.when(k >= 2)
        def _():
            load(e, g, me).wait()
            local(e, g).wait()

        keep(e, g, g)
        refill(k, me)

    if experts > 1:
        each(experts - 1, more)

    each(m - 1, lambda j: group_copy(mate(j), mate(j)).wait_recv())
    lines = rbuf.shape[1]
    for g in range(m):
        rwide[g * lines:(g + 1) * lines, :] = rbuf[g].astype(jnp.float32)
    router_v[...] = rwide[...].astype(jnp.bfloat16)
    for e in range(experts):
        sc_v[e:e + 1, :] = sc_rows[e]
    put_router = pltpu.make_async_copy(router_v, router, out_sem.at[0])
    put_scale = pltpu.make_async_copy(sc_v, sc, out_sem.at[1])
    put_router.start()
    put_scale.start()

    for s in range(min(experts, 2)):
        local(0, s).wait()

    def finish(j):
        d = peer(j)
        for t in range(leads):
            early_copy(t, d, me).wait_send()
        router_copy(d, me).wait_send()
        for p in range(len(pieces)):
            piece_copy(p, j, d, me).wait_send()
            piece_copy(p, j, d, d).wait_recv()
        if rest:
            @pl.when(d % half != rank)
            def _():
                sums(0, d, rank).wait_send()

            bulk_rest(j, d, me).wait_send()
            bulk_rest(j, d, d).wait_recv()

        def others(k):
            e = k + 1

            @pl.when(d % half != rank)
            def _():
                sums(e, d, rank).wait_send()

            cut = (e == last) & (j == far)

            @pl.when(cut)
            def _():
                bulk_short(d, me).wait_send()
                bulk_short(d, d).wait_recv()

            @pl.when(jnp.logical_not(cut))
            def _():
                bulk(e, j, d, me).wait_send()
                bulk(e, j, d, d).wait_recv()

        if experts > 1:
            each(experts - 1, others)

    each(n - 1, finish)
    each(half - 1, lambda j: scale_copy(other(j), rank).wait_send())
    across(side).wait_send()
    each(m - 1, lambda j: group_copy(mate(j), group).wait_send())
    put_router.wait()
    put_scale.wait()
    to_tail().wait()


def exchange(n, m, w, rw, gain):
    experts, rows, cols = w.shape
    lines, width = rw.shape
    block = rows // n
    tiles = -(-block // LANES)
    padded = ceil_to(tiles, 8)
    depth = ceil_to(n, 8)
    leads = min(LEADS, tiles)
    keep_back = tail_rows(block)
    pieces = len(cuts(min(leads * LANES, block)))
    dma = pltpu.SemaphoreType.DMA
    f32, bf16 = jnp.float32, jnp.bfloat16
    buffers = [
        ((2, n, block, cols), f32),
        ((experts, n - 1, block, cols), bf16),
        ((2, block, cols), bf16),
        ((leads, n, depth, LANES), f32),
        ((leads, 2, depth, LANES), f32),
        ((experts, n, padded, LANES), f32),
        ((experts, n // 2, 2, padded, LANES), f32),
        ((2, experts, 2, padded, LANES), f32),
        ((n // 2, experts, 2, padded, LANES), f32),
        ((lines, width), f32),
        ((1, width), f32),
        ((m, lines, n * width), bf16),
        ((m * lines, n * width), f32),
        ((m * lines, n * width), bf16),
        ((experts, block), f32),
        ((experts, 1, block), f32),
    ]
    return pl.pallas_call(
        functools.partial(kernel, n, m),
        out_shape=(
            jax.ShapeDtypeStruct((experts, block, n * cols), bf16),
            jax.ShapeDtypeStruct((experts, block), f32),
            jax.ShapeDtypeStruct((m * lines, n * width), bf16),
            jax.ShapeDtypeStruct((keep_back, cols), bf16),
        ),
        in_specs=[pl.BlockSpec(memory_space=pltpu.HBM)] * 3,
        out_specs=(pl.BlockSpec(memory_space=pl.ANY),) * 4,
        scratch_shapes=[pltpu.VMEM(s, t) for s, t in buffers] + [
            dma((leads, n)), dma((2, n)), dma((2,)), dma((leads, n)), dma((leads, n)),
            dma((experts, n)), dma((experts, n)), dma, dma, dma((n,)), dma((n,)),
            dma((pieces, n)), dma((pieces, n)), dma((experts, n)), dma((experts, n)), dma((2,)),
            dma((n,)), dma((n,)), dma((m,)), dma((m,)), dma((3,)),
        ],
        compiler_params=pltpu.CompilerParams(
            collective_id=0, has_side_effects=True,
            vmem_limit_bytes=VMEM_BYTES),
    )(w, rw, gain)


def tail_rows(block):
    start = ceil_to(block * TAIL_START // 100, 16)
    return block - start


def settle_kernel(o, sc, router, full, sc_out, router_out, buf, sc_v, router_v, get, put):
    experts, block, _ = o.shape
    parts = get.shape[0] - 1
    rows = block * experts // (parts - 1)
    per = block // rows
    pairs = [(sc, sc_v, sc_out), (router, router_v, router_out)]

    def where(i):
        return i // per, pl.ds(pl.multiple_of(i % per * rows, 8), rows)

    def load(i):
        e, r = where(i)
        return pltpu.make_async_copy(o.at[e, r, :], buf.at[e, r, :], get.at[i])

    def save(i):
        e, r = where(i)
        return pltpu.make_async_copy(buf.at[e, r, :], full.at[e, r, :], put.at[i])

    def load_small(i):
        return pltpu.make_async_copy(pairs[i][0], pairs[i][1], get.at[parts - 1 + i])

    def save_small(i):
        return pltpu.make_async_copy(pairs[i][1], pairs[i][2], put.at[parts - 1 + i])

    each(parts - 1, lambda i: load(i).start())
    for i in range(2):
        load_small(i).start()

    def move(i):
        load(i).wait()
        save(i).start()

    each(parts - 1, move)
    for i in range(2):
        load_small(i).wait()
        save_small(i).start()
    each(parts - 1, lambda i: save(i).wait())
    for i in range(2):
        save_small(i).wait()


def settle(o, sc, router):
    experts, block, _ = o.shape
    per = max(p for p in (1, 2, 4, 5) if p == 1 or block % (16 * p) == 0)
    count = experts * per + 2
    dma = pltpu.SemaphoreType.DMA
    return pl.pallas_call(
        settle_kernel,
        out_shape=tuple(jax.ShapeDtypeStruct(a.shape, a.dtype) for a in (o, sc, router)),
        in_specs=[pl.BlockSpec(memory_space=pltpu.HBM)] * 3,
        out_specs=(pl.BlockSpec(memory_space=pltpu.HBM),) * 3,
        scratch_shapes=[pltpu.VMEM(a.shape, a.dtype) for a in (o, sc, router)] + [
            dma((count,)), dma((count,))],
        cost_estimate=pl.CostEstimate(flops=0, bytes_accessed=4 * o.size, transcendentals=0),
        compiler_params=pltpu.CompilerParams(vmem_limit_bytes=48 * 1024 * 1024),
    )(o, sc, router)


def place_kernel(n, expert, full, got, out, sem):
    del full
    rows, cols = got.shape
    source = (lax.axis_index("fsdp") + n // 2) % n
    copy = pltpu.make_async_copy(
        got, out.at[expert, pl.ds(out.shape[1] - rows, rows),
                    pl.ds(pl.multiple_of(source * cols, LANES), cols)], sem)
    copy.start()
    copy.wait()


def place(n, expert, full, got):
    return pl.pallas_call(
        functools.partial(place_kernel, n, expert),
        out_shape=jax.ShapeDtypeStruct(full.shape, full.dtype),
        in_specs=[pl.BlockSpec(memory_space=pltpu.HBM), pl.BlockSpec(memory_space=pltpu.VMEM)],
        out_specs=pl.BlockSpec(memory_space=pltpu.HBM),
        scratch_shapes=[pltpu.SemaphoreType.DMA],
        input_output_aliases={0: 0},
        compiler_params=pltpu.CompilerParams(vmem_limit_bytes=8 * 1024 * 1024),
    )(full, got)


def body(n, m, w_down, router_weight, router_gain):
    experts = w_down.shape[0]
    o, scale, router, tail = exchange(n, m, w_down, router_weight.T, router_gain[None, :])
    got = lax.ppermute(tail, "fsdp", [(i, (i + n // 2) % n) for i in range(n)])
    full, scale, router = settle(o, scale, router)
    serve_down = place(n, experts - 2 if experts > 2 else 1, full, got)
    return (serve_down, scale, router.T)


def solution(mesh):
    in_specs = (P("ep", None, "fsdp"), P("fsdp", "ep"), P("fsdp"))
    out_specs = (P("ep", "fsdp", None), P("ep", "fsdp"), P())
    return jax.shard_map(
        functools.partial(body, mesh.shape["fsdp"], mesh.shape["ep"]), mesh=mesh,
        in_specs=in_specs, out_specs=out_specs, check_vma=False)
```
